32 devices in a mesh: pipe: 2 (over core), dp: 4 (over z), mp: 4 (over y, x).
Axes of the slice: x: 2, y: 2, z: 4, core: 2. Of those that a mesh axis runs over, the one named last changes fastest.
Arguments:
- hidden_states: bfloat16 [16, 64, 4096], P('dp'), may hold values from -6 to 6
- up_weight: bfloat16 [2, 4096, 7168], P('pipe', 'dp', 'mp'), may hold values from -0.09375 to 0.09375
- down_weight: bfloat16 [2, 7168, 4096], P('pipe', 'mp', 'dp'), may hold values from -0.0625 to 0.0625
- layer_gain: float32 [2, 4096], P('pipe'), may hold values from 0.5 to 1.5
- final_gain: float32 [4096], replicated, may hold values from 0.5 to 1.5
- unembedding: bfloat16 [32768, 4096], P(('pipe', 'mp')), may hold values from -32 to 32
- target_ids: int32 [16, 64], P('dp'), may hold values from 0 to 32767
- response_masks: int32 [16, 64], P('dp'), may hold values from 0 to 1, as said below
- anchor_logps: float32 [16, 64], P('dp'), may hold values from -14 to -10
- pairing: int32 [4, 4], P('dp'), may hold values from 0 to 3, each once within a row
Outputs:
- token_logps: float32 [16, 64], P('dp')
- seq_logps: float32 [16], P('dp')
- pair_losses: float32 [8], P('dp')
The draws below stay inside these ranges and needn't reach their ends.
Inputs may be any that keep to these rules, and one draw needn't show every extreme that they name: response_masks is 1 on one unbroken run of at least one position per sequence, starting at or after position 8, and 0 elsewhere.
All inputs are finite; a program needn't handle non-finite values.
Results may differ from the reference program's by a relative error of at most 0.0075.
Values may be sent and summed in bfloat16 or wider, within the bound.
A program may use at most 192 MiB of HBM per device.

```python
import math
import jax
import jax.numpy as jnp
import numpy as np
from jax import lax

D = 4096
VOCAB = 32768
FF = 7168
LEN = 64
SEQ_DEV = 4
SEQ_MB = 1
MICRO = 4
GROUPS = 4
SEQS = 16
PAIRS = 8
SECTIONS = 2


def draw_unembedding(key, part):
    values = jax.random.normal(key, (VOCAB, D), jnp.float32) * (2.0 * D ** (-0.5))
    values = jnp.clip(values, -12.0 * D ** (-0.5), 12.0 * D ** (-0.5))
    return values.astype(jnp.bfloat16)


def draw_response_masks(key, part):
    first_key, second_key = jax.random.split(key)
    starts = jax.random.randint(first_key, (SEQS, 1), LEN // 8, LEN // 2)
    spread = jax.random.randint(second_key, (SEQS, 1), 0, 1 << 20)
    spans = 1 + spread % (LEN - starts)
    positions = jnp.arange(LEN, dtype=jnp.int32)[None, :]
    return ((positions >= starts) & (positions < starts + spans)).astype(jnp.int32)


def set_ends(array, key, low, largest):
    spot = [jax.random.randint(jax.random.fold_in(key, axis), (), 0, length) for axis, length in enumerate(array.shape)]
    main_axis = array.shape.index(max(array.shape))
    next_to = spot[:main_axis] + [(spot[main_axis] + 1) % array.shape[main_axis]] + spot[main_axis + 1:]
    return array.at[tuple(spot)].set(low).at[tuple(next_to)].set(largest)


def steps_of(key, dims, cuts, low, largest):
    def one(axis_at, parts):
        heights = jax.random.uniform(jax.random.fold_in(jax.random.fold_in(key, 6), axis_at), (parts,), jnp.float32, low / len(cuts), largest / len(cuts))
        return jnp.repeat(jnp.exp(heights), dims[axis_at] // parts).reshape((-1,) + (1,) * (len(dims) - axis_at - 1))

    gain = one(*cuts[0])
    for cut in cuts[1:]:
        gain = gain * one(*cut)
    return gain


def rank_table(count, lean):
    portions = [(1 << 20) // math.isqrt(grade ** lean) + 1 for grade in range(1, count + 1)]
    scale = 1 + sum(portions) // (1 << 30)
    return np.cumsum(np.array([max(1, weight // scale) for weight in portions]))


def ranked_ids(rng, dims, amount, skew):
    table = rank_table(amount, skew)
    lot = jax.random.randint(jax.random.fold_in(rng, 1), dims, 0, int(table[amount - 1]))
    standing = jnp.searchsorted(jnp.asarray(table, jnp.int32), lot, side="right")
    return jax.random.permutation(jax.random.fold_in(rng, 2), amount)[standing].astype(jnp.int32)


def normal_values(own_key, dims, width, most, shards=(), kind=jnp.bfloat16):
    values = jax.random.normal(own_key, dims, jnp.float32) * width
    if len(shards) > 0:
        values = steps_of(own_key, dims, shards, -0.22, 0.18) * values
    return jnp.clip(values, min=-most, max=most).astype(kind)


def setup_inputs(seed: int = 0) -> dict:
    key_list = jax.random.split(jax.random.key(seed), 11)
    hidden_states = normal_values(key_list[0], (SEQS, LEN, D), 1.0, 6.0, ((0, 4),))
    up_weight = normal_values(key_list[1], (SECTIONS, D, FF), D ** -0.5, 0.09375, ((0, 2), (1, 4), (2, 4)))
    down_weight = normal_values(key_list[2], (SECTIONS, FF, D), FF ** -0.5, 0.0625, ((0, 2), (1, 4), (2, 4)))
    layer_gain = jnp.clip(1.0 + 0.1 * jax.random.normal(key_list[3], (SECTIONS, D), jnp.float32), 0.5, 1.5)
    final_gain = jnp.clip(1.0 + 0.1 * jax.random.normal(key_list[4], (D,), jnp.float32), 0.5, 1.5)
    unembedding = draw_unembedding(jax.random.fold_in(key_list[10], 71), 0)
    target_ids = set_ends(ranked_ids(key_list[6], (SEQS, LEN), VOCAB, 2), jax.random.fold_in(key_list[6], 3), 0, VOCAB - 1).astype(jnp.int32)
    response_masks = draw_response_masks(jax.random.fold_in(key_list[10], 71), 0)
    anchor_logps = jnp.clip(-14.0 + 4.0 * jax.random.uniform(key_list[8], (SEQS, LEN), jnp.float32) ** steps_of(key_list[8], (SEQS, LEN), ((0, 4),), -0.2, 0.2), -14.0, -10.0)
    pairing = jax.vmap(lambda own: jax.random.permutation(own, SEQ_DEV))(jax.random.split(key_list[9], GROUPS)).reshape((GROUPS, SEQ_DEV)).astype(jnp.int32)
    return dict(hidden_states=hidden_states, up_weight=up_weight, down_weight=down_weight, layer_gain=layer_gain, final_gain=final_gain, unembedding=unembedding, target_ids=target_ids, response_masks=response_masks, anchor_logps=anchor_logps, pairing=pairing)


epsilon = 1e-05
ipo_tau = 0.5

def rms_scale(values, gain_row):
    mean_square = lax.optimization_barrier(jnp.mean(values * values, axis=-1, keepdims=True))
    return values * lax.rsqrt(mean_square + epsilon) * gain_row.astype(jnp.float32)

def section_layer(states, gain_row, up_matrix, down_matrix):
    wide_states = states.astype(jnp.float32)
    normed = rms_scale(wide_states, gain_row).astype(jnp.bfloat16)
    active = jax.nn.silu(jnp.dot(normed, up_matrix, preferred_element_type=jnp.float32)).astype(jnp.bfloat16)
    summed = wide_states + jnp.dot(active, down_matrix, preferred_element_type=jnp.float32)
    return summed.astype(jnp.bfloat16)

def token_scores(finals, final_gain, unembedding, wanted_ids):
    normed = rms_scale(finals.astype(jnp.float32), final_gain).astype(jnp.bfloat16)
    logits = jnp.dot(normed, unembedding.T, preferred_element_type=jnp.float32)
    top_value = lax.optimization_barrier(jnp.max(logits, axis=1, keepdims=True))
    log_total = top_value[:, 0] + jnp.log(lax.optimization_barrier(jnp.sum(jnp.exp(logits - top_value), axis=1)))
    picked = jnp.take_along_axis(logits, wanted_ids[:, None], axis=1)[:, 0]
    return picked - log_total

def reference(hidden_states, up_weight, down_weight, layer_gain, final_gain, unembedding, target_ids, response_masks, anchor_logps, pairing):

    def one_group(group_items):
        states, wanted_ids = group_items
        flat_states = states.reshape(SEQ_DEV * LEN, D)
        for section_index in range(SECTIONS):
            flat_states = section_layer(flat_states, layer_gain[section_index], up_weight[section_index], down_weight[section_index])
        return token_scores(flat_states, final_gain, unembedding, wanted_ids.reshape(SEQ_DEV * LEN)).reshape(SEQ_DEV, LEN)
    token_logps = lax.map(one_group, (hidden_states.reshape(GROUPS, SEQ_DEV, LEN, D), target_ids.reshape(GROUPS, SEQ_DEV, LEN)))
    token_logps = token_logps.reshape(SEQS, LEN)
    mask_values = response_masks.astype(jnp.float32)
    counts = lax.optimization_barrier(jnp.sum(mask_values.reshape(GROUPS, MICRO, SEQ_MB * LEN), axis=(0, 2)))
    mean_length = counts / (GROUPS * SEQ_MB)
    divisor = jnp.tile(jnp.repeat(mean_length, SEQ_MB), GROUPS)
    policy = lax.optimization_barrier(jnp.sum(mask_values * token_logps, axis=1)) / divisor
    anchor = lax.optimization_barrier(jnp.sum(mask_values * anchor_logps, axis=1)) / divisor
    log_gaps = (policy - anchor).reshape(GROUPS, SEQ_DEV)
    chosen = jnp.take_along_axis(log_gaps, pairing[:, 0::2], axis=1)
    rejected = jnp.take_along_axis(log_gaps, pairing[:, 1::2], axis=1)
    losses = (chosen - rejected - 0.5 / ipo_tau) ** 2
    return (token_logps, policy, losses.reshape(PAIRS))
```

```python
import jax
import jax.numpy as jnp
from jax import lax
from jax.sharding import PartitionSpec as P

SEQ_MB = 1

epsilon = 1e-05
ipo_tau = 0.5
VP = ("pipe", "mp")


def shards(
    hidden_states,
    up_weight,
    down_weight,
    layer_gain,
    final_gain,
    unembedding,
    target_ids,
    response_masks,
    anchor_logps,
    pairing,
):
    seq_count, length, model_width = hidden_states.shape
    groups = lax.axis_size("dp")
    vp_size = lax.axis_size("pipe") * lax.axis_size("mp")
    vp_index = lax.axis_index(VP)
    dp_index = lax.axis_index("dp")
    pipe_index = lax.axis_index("pipe")
    rows = seq_count * length
    part = rows // vp_size
    block = model_width // groups
    mask_values = response_masks.astype(jnp.float32)
    local_counts = jnp.sum(mask_values, axis=1)
    counts = lax.psum(local_counts, "dp")

    up_own, down_own = up_weight[0], down_weight[0]
    half = up_own.shape[1] // 2
    away = (1 - pipe_index) * half
    keep = pipe_index * half
    swap = [(0, 1), (1, 0)]
    gain_other = lax.ppermute(layer_gain, "pipe", swap)
    up_other = lax.ppermute(lax.dynamic_slice_in_dim(up_own, away, half, 1), "pipe", swap)
    down_other = lax.ppermute(lax.dynamic_slice_in_dim(down_own, away, half, 0), "pipe", swap)
    up_mine = lax.dynamic_slice_in_dim(up_own, keep, half, 1)
    down_mine = lax.dynamic_slice_in_dim(down_own, keep, half, 0)

    def section_of(s):
        own = pipe_index == s
        gain = jnp.where(own, layer_gain[0], gain_other[0])
        return (
            lax.dynamic_slice_in_dim(gain, dp_index * block, block, 0),
            jnp.where(own, up_mine, up_other),
            jnp.where(own, down_mine, down_other),
        )

    mine = lax.dynamic_slice_in_dim(
        hidden_states.reshape(rows, model_width), vp_index * part, part, 0
    )
    blocks = lax.all_to_all(
        mine.reshape(part, groups, block).transpose(1, 0, 2), "dp", 0, 0, tiled=True
    ).reshape(groups * part, block)

    for s in range(2):
        gain, up, down = section_of(s)
        wide = blocks.astype(jnp.float32)
        total = lax.psum(jnp.sum(wide * wide, axis=1, keepdims=True), "dp")
        normed = (wide * lax.rsqrt(total / model_width + epsilon) * gain).astype(jnp.bfloat16)
        full = lax.all_gather(normed, VP, axis=0, tiled=True)
        hidden = jnp.dot(full, up, preferred_element_type=jnp.float32).astype(jnp.bfloat16)
        hidden = lax.psum_scatter(hidden, "dp", scatter_dimension=0, tiled=True)
        active = jax.nn.silu(hidden.astype(jnp.float32)).astype(jnp.bfloat16)
        active = lax.all_gather(active, "dp", axis=0, tiled=True)
        out = jnp.dot(active, down, preferred_element_type=jnp.float32).astype(jnp.bfloat16)
        out = lax.psum_scatter(out, VP, scatter_dimension=0, tiled=True)
        blocks = (wide + out.astype(jnp.float32)).astype(jnp.bfloat16)

    finals = lax.all_to_all(blocks.reshape(groups, part, block), "dp", 0, 0, tiled=True)
    finals = finals.transpose(1, 0, 2).reshape(part, model_width).astype(jnp.float32)
    mean_square = jnp.mean(finals * finals, axis=-1, keepdims=True)
    normed_final = (finals * lax.rsqrt(mean_square + epsilon) * final_gain).astype(jnp.bfloat16)
    normed_final = lax.all_gather(normed_final, VP, axis=0, tiled=True)
    logits = lax.dot_general(
        normed_final, unembedding, (((1,), (1,)), ((), ())), preferred_element_type=jnp.float32
    )
    vocab_start = vp_index * unembedding.shape[0]
    local_ids = target_ids.reshape(-1) - vocab_start
    columns = lax.broadcasted_iota(jnp.int32, logits.shape, 1)
    picked = jnp.sum(jnp.where(columns == local_ids[:, None], logits, 0.0), axis=1)
    local_top = jnp.max(logits, axis=1)
    local_sum = jnp.sum(jnp.exp(logits - local_top[:, None]), axis=1)
    stats = lax.all_gather(jnp.stack([local_top, local_sum, picked]), VP, axis=0)
    top_value = jnp.max(stats[:, 0], axis=0)
    exp_total = jnp.sum(stats[:, 1] * jnp.exp(stats[:, 0] - top_value), axis=0)
    picked_all = jnp.sum(stats[:, 2], axis=0)
    token_logps = (picked_all - top_value - jnp.log(exp_total)).reshape(seq_count, length)

    divisor = jnp.repeat(counts / (groups * SEQ_MB), SEQ_MB)
    policy = jnp.sum(mask_values * token_logps, axis=1) / divisor
    anchor = jnp.sum(mask_values * anchor_logps, axis=1) / divisor
    log_gaps = policy - anchor
    positions = jnp.arange(seq_count, dtype=jnp.int32)
    chosen = jnp.sum(
        jnp.where(pairing[0, 0::2][:, None] == positions[None, :], log_gaps[None, :], 0.0), axis=1
    )
    rejected = jnp.sum(
        jnp.where(pairing[0, 1::2][:, None] == positions[None, :], log_gaps[None, :], 0.0), axis=1
    )
    losses = (chosen - rejected - 0.5 / ipo_tau) ** 2
    return (token_logps, policy, losses)


def solution(mesh):
    return jax.shard_map(
        shards,
        mesh=mesh,
        in_specs=(
            P("dp", None, None),
            P("pipe", "dp", "mp"),
            P("pipe", "mp", "dp"),
            P("pipe", None),
            P(),
            P(("pipe", "mp"), None),
            P("dp", None),
            P("dp", None),
            P("dp", None),
            P("dp", None),
        ),
        out_specs=(P("dp", None), P("dp"), P("dp")),
        check_vma=False,
    )
```

```python
import functools
import jax
import jax.numpy as jnp
from jax import lax
from jax.experimental import pallas as pl
from jax.experimental.pallas import tpu as pltpu
from jax.sharding import PartitionSpec as P

SEQ_MB = 1

epsilon = 1e-05
ipo_tau = 0.5
VP = ("pipe", "mp")
MESH = pl.DeviceIdType.MESH
PIECES = 8


def remote(src, dst, send_sem, recv_sem, target):
    return pltpu.make_async_remote_copy(
        src_ref=src,
        dst_ref=dst,
        send_sem=send_sem,
        recv_sem=recv_sem,
        device_id=target,
        device_id_type=MESH,
    )


def greet(axes):
    barrier = pltpu.get_barrier_semaphore()
    total = 0
    for axis in axes:
        size = lax.axis_size(axis)
        here = lax.axis_index(axis)
        for k in range(1, size):
            pl.semaphore_signal(
                barrier, inc=1, device_id={axis: lax.rem(here + k, size)}, device_id_type=MESH
            )
        total += size - 1
    pl.semaphore_wait(barrier, total)


def chunk_rows(index, size):
    return pl.ds(pl.multiple_of(index * size, 8), size)


def spread(full, size, mp_sems, pipe_sems):
    (mp_send, mp_recv), (pipe_send, pipe_recv) = mp_sems, pipe_sems
    count = lax.axis_size("mp")
    m, p = lax.axis_index("mp"), lax.axis_index("pipe")

    def to_mp(k, owner):
        rows = full.at[chunk_rows(p * count + owner, size)]
        return remote(rows, rows, mp_send.at[k], mp_recv.at[k], {"mp": lax.rem(m + k, count)})

    def to_pipe(k, pipe):
        rows = full.at[chunk_rows(pipe * count + lax.rem(m - k + count, count), size)]
        return remote(rows, rows, pipe_send.at[k], pipe_recv.at[k], {"pipe": 1 - p})

    for k in range(1, count):
        to_mp(k, m).start()
    to_pipe(0, p).start()
    for k in range(1, count):
        to_mp(k, lax.rem(m - k + count, count)).wait_recv()
        to_pipe(k, p).start()
    for k in range(count):
        to_pipe(k, 1 - p).wait_recv()
    for k in range(1, count):
        to_mp(k, m).wait_send()
    for k in range(count):
        to_pipe(k, p).wait_send()


def gather_sum(part, size, near, far, sent, sems):
    near_send, near_recv, far_send, far_recv = sems
    count = lax.axis_size("mp")
    m, p = lax.axis_index("mp"), lax.axis_index("pipe")
    order = list(range(1, count)) + [0]

    def to_core(k):
        rows = part.at[chunk_rows((1 - p) * count + lax.rem(m + k, count), size)]
        return remote(rows, near.at[k], near_send.at[k], near_recv.at[k], {"pipe": 1 - p})

    def to_chip(k):
        return remote(
            sent.at[k], far.at[k], far_send.at[k], far_recv.at[k], {"mp": lax.rem(m + k, count)}
        )

    for k in order:
        to_core(k).start()
    for k in order:
        to_core(k).wait_recv()
        own = part[chunk_rows(p * count + lax.rem(m + k, count), size), :].astype(jnp.float32)
        own = own + near[k].astype(jnp.float32)
        if k > 0:
            sent[k] = own.astype(sent.dtype)
            to_chip(k).start()
    for k in range(1, count):
        to_chip(k).wait_recv()
        own = own + far[k].astype(jnp.float32)
    for k in range(1, count):
        to_chip(k).wait_send()
    for k in order:
        to_core(k).wait_send()
    return own


def share_sum(slots, send, recv):
    count = lax.axis_size("dp")
    d = lax.axis_index("dp")

    def hop(k):
        return remote(
            slots.at[0], slots.at[k], send.at[k], recv.at[k], {"dp": lax.rem(d + k, count)}
        )

    for k in range(1, count):
        hop(k).start()
    total = slots[0]
    for k in range(1, count):
        hop(k).wait_recv()
        total = total + slots[k]
    for k in range(1, count):
        hop(k).wait_send()
    return total


def first_kernel(
    x_ref, gain_ref, blocks_ref, full_ref, normed_ref, n_send, n_recv, x_send, x_recv, ms, mr, ps, pr
):
    count = lax.axis_size("dp")
    d = lax.axis_index("dp")
    v = lax.axis_index(("pipe", "mp"))
    part, width = x_ref.shape
    block = width // count
    greet(("dp", "mp", "pipe"))
    wide = x_ref[...].astype(jnp.float32)
    scale = lax.rsqrt(jnp.mean(wide * wide, axis=-1, keepdims=True) + epsilon)
    normed_ref[...] = (wide * scale * gain_ref[...]).astype(normed_ref.dtype)

    def columns(owner):
        return pl.ds(pl.multiple_of(owner * block, 128), block)

    def normed_hop(k, owner):
        to = lax.rem(d + k, count)
        return remote(
            normed_ref.at[:, columns(to)],
            full_ref.at[chunk_rows(v * count + owner, part)],
            n_send.at[k],
            n_recv.at[k],
            {"dp": to},
        )

    def plain_hop(k, owner):
        to = lax.rem(d + k, count)
        return remote(
            x_ref.at[:, columns(to)],
            blocks_ref.at[chunk_rows(owner, part)],
            x_send.at[k],
            x_recv.at[k],
            {"dp": to},
        )

    for k in range(1, count):
        normed_hop(k, d).start()
    for k in range(1, count):
        plain_hop(k, d).start()
    full_ref[chunk_rows(v * count + d, part), :] = normed_ref[:, columns(d)]
    blocks_ref[chunk_rows(d, part), :] = x_ref[:, columns(d)]
    for k in range(1, count):
        normed_hop(k, lax.rem(d - k + count, count)).wait_recv()
    spread(full_ref, part * count, (ms, mr), (ps, pr))
    for k in range(1, count):
        plain_hop(k, lax.rem(d - k + count, count)).wait_recv()
    for k in range(1, count):
        normed_hop(k, d).wait_send()
        plain_hop(k, d).wait_send()


def middle_kernel(
    width, part_ref, resid_ref, gain_ref, blocks_ref, full_ref,
    near, far, sent, slots, ns, nr, fs, fr, qs, qr, ms, mr, ps, pr,
):
    v = lax.axis_index(("pipe", "mp"))
    size = resid_ref.shape[0]
    greet(("dp", "mp", "pipe"))
    summed = gather_sum(part_ref, size, near, far, sent, (ns, nr, fs, fr))
    value = (resid_ref[...].astype(jnp.float32) + summed).astype(jnp.bfloat16)
    blocks_ref[...] = value
    wide = value.astype(jnp.float32)
    slots[0] = lax.dot_general(
        jnp.ones((8, wide.shape[1]), jnp.float32),
        wide * wide,
        (((1,), (1,)), ((), ())),
        precision=lax.Precision.HIGHEST,
        preferred_element_type=jnp.float32,
    )
    scale = lax.rsqrt(share_sum(slots, qs, qr) / width + epsilon)
    scale = jnp.transpose(scale)[:, :1]
    wide = blocks_ref[...].astype(jnp.float32)
    full_ref[chunk_rows(v, size), :] = (wide * scale * gain_ref[...]).astype(full_ref.dtype)
    spread(full_ref, size, (ms, mr), (ps, pr))


def last_kernel(
    part_ref, resid_ref, gain_ref, full_ref,
    near, far, sent, blocks, fin, ns, nr, fs, fr, hs, hr, ms, mr, ps, pr,
):
    count = lax.axis_size("dp")
    d = lax.axis_index("dp")
    v = lax.axis_index(("pipe", "mp"))
    size, block = resid_ref.shape
    part = size // count
    greet(("dp", "mp", "pipe"))
    summed = gather_sum(part_ref, size, near, far, sent, (ns, nr, fs, fr))
    blocks[...] = (resid_ref[...].astype(jnp.float32) + summed).astype(jnp.bfloat16)

    def hop(k, owner):
        to = lax.rem(d + k, count)
        return remote(
            blocks.at[chunk_rows(to, part)], fin.at[owner], hs.at[k], hr.at[k], {"dp": to}
        )

    for k in range(1, count):
        hop(k, d).start()
    fin[d] = blocks[chunk_rows(d, part), :]
    for k in range(1, count):
        hop(k, lax.rem(d - k + count, count)).wait_recv()
    total = 0.0
    for g in range(count):
        wide = fin[g].astype(jnp.float32)
        total = total + jnp.sum(wide * wide, axis=1, keepdims=True)
    scale = lax.rsqrt(total / (block * count) + epsilon)
    for g in range(count):
        cut = slice(g * block, (g + 1) * block)
        full_ref[chunk_rows(v, part), cut] = (
            fin[g].astype(jnp.float32) * scale * gain_ref[:, cut]
        ).astype(full_ref.dtype)
    spread(full_ref, part, (ms, mr), (ps, pr))
    for k in range(1, count):
        hop(k, d).wait_send()


def stats_kernel(stats_ref, counts_ref, full_ref, total_ref, slots, qs, qr, ms, mr, ps, pr):
    v = lax.axis_index(("pipe", "mp"))
    size = stats_ref.shape[0]
    greet(("dp", "mp", "pipe"))
    slots[0] = counts_ref[...]
    full_ref[chunk_rows(v, size), :] = stats_ref[...]
    total_ref[...] = share_sum(slots, qs, qr)
    spread(full_ref, size, (ms, mr), (ps, pr))


def chain_kernel(h_ref, out_ref, arrived, summed, rs, rr, gs, gr):
    count = lax.axis_size("dp")
    d = lax.axis_index("dp")
    half = h_ref.shape[0] // 2
    rows = half // PIECES
    right, left = lax.rem(d + 1, count), lax.rem(d + count - 1, count)
    barrier = pltpu.get_barrier_semaphore()
    for has, who in ((d > 0, left), (d < count - 1, right)):

        @pl.when(has)
        def _():
            pl.semaphore_signal(barrier, inc=1, device_id={"dp": who}, device_id_type=MESH)

    ends = (d > 0).astype(jnp.int32) + (d < count - 1).astype(jnp.int32)
    pl.semaphore_wait(barrier, ends)

    hops = (d, count - 1 - d)

    def cut(way, c):
        return pl.ds(pl.multiple_of((1 - way) * half + c * rows, 16), rows)

    def onward_copy(way, c, source):
        to = (right, left)[way]
        return remote(source, arrived.at[way, c], rs.at[way, c], rr.at[way, c], {"dp": to})

    def back_copy(way, c):
        spot = out_ref.at[cut(way, c)]
        to = (left, right)[way]
        return remote(spot, spot, gs.at[way, c], gr.at[way, c], {"dp": to})

    for way in range(2):

        @pl.when(hops[way] == 0)
        def _():
            for c in range(PIECES):
                onward_copy(way, c, h_ref.at[cut(way, c)]).start()

    def step(t, carry):
        for way in range(2):
            before = hops[way]
            c = t - before

            @pl.when((before > 0) & (c >= 0) & (c < PIECES))
            def _():
                onward_copy(way, c, summed.at[way, c]).wait_recv()
                total = arrived[way, c] + h_ref[cut(way, c), :]

                @pl.when(before < count - 1)
                def _():
                    summed[way, c] = total
                    onward_copy(way, c, summed.at[way, c]).start()

                @pl.when(before == count - 1)
                def _():
                    out_ref[cut(way, c), :] = (total / (1.0 + jnp.exp(-total))).astype(
                        out_ref.dtype
                    )
                    back_copy(way, c).start()

        for way in range(2):
            after = count - 1 - hops[way]
            g = t - (count - 1) - after

            @pl.when((after > 0) & (g >= 0) & (g < PIECES))
            def _():
                back_copy(way, g).wait_recv()

                @pl.when(after < count - 1)
                def _():
                    back_copy(way, g).start()

        return carry

    lax.fori_loop(0, PIECES + 2 * (count - 1), step, 0)
    for way in range(2):

        @pl.when(hops[way] < count - 1)
        def _():
            for c in range(PIECES):
                onward_copy(way, c, summed.at[way, c]).wait_send()

        @pl.when(hops[way] > 0)
        def _():
            for c in range(PIECES):
                back_copy(way, c).wait_send()


def call(kernel, name, ident, outs, scratch, *args):
    spec = pl.BlockSpec(memory_space=pltpu.VMEM)
    return pl.pallas_call(
        kernel,
        name=name,
        out_shape=outs,
        in_specs=[spec] * len(args),
        out_specs=jax.tree.map(lambda _: spec, outs),
        scratch_shapes=scratch,
        compiler_params=pltpu.CompilerParams(collective_id=ident, has_side_effects=True),
    )(*args)


def sems(*shape):
    return [pltpu.SemaphoreType.DMA(shape)] * 2


def shards(
    hidden_states,
    up_weight,
    down_weight,
    layer_gain,
    final_gain,
    unembedding,
    target_ids,
    response_masks,
    anchor_logps,
    pairing,
):
    seq_count, length, model_width = hidden_states.shape
    groups = lax.axis_size("dp")
    vp_size = lax.axis_size("pipe") * lax.axis_size("mp")
    vp_index = lax.axis_index(VP)
    dp_index = lax.axis_index("dp")
    pipe_index = lax.axis_index("pipe")
    rows = seq_count * length
    part = rows // vp_size
    block = model_width // groups
    mask_values = response_masks.astype(jnp.float32)
    local_counts = jnp.sum(mask_values, axis=1)
    count = lax.axis_size("mp")
    bf16 = jnp.bfloat16
    spread_sems = sems(count) + sems(count)
    reach_sems = sems(count) + sems(count)
    buffers = [pltpu.VMEM((count, part, block), jnp.float32) for part in [rows // vp_size * groups]] * 3

    up_own, down_own = up_weight[0], down_weight[0]
    half = up_own.shape[1] // 2
    away = (1 - pipe_index) * half
    keep = pipe_index * half
    swap = [(0, 1), (1, 0)]
    gain_other = lax.ppermute(layer_gain, "pipe", swap)
    up_other = lax.ppermute(lax.dynamic_slice_in_dim(up_own, away, half, 1), "pipe", swap)
    down_other = lax.ppermute(lax.dynamic_slice_in_dim(down_own, away, half, 0), "pipe", swap)
    up_mine = lax.dynamic_slice_in_dim(up_own, keep, half, 1)
    down_mine = lax.dynamic_slice_in_dim(down_own, keep, half, 0)

    def section_of(s):
        own = pipe_index == s
        gain = jnp.where(own, layer_gain[0], gain_other[0])
        return (
            lax.dynamic_slice_in_dim(gain, dp_index * block, block, 0),
            jnp.where(own, up_mine, up_other),
            jnp.where(own, down_mine, down_other),
        )

    mine = lax.dynamic_slice_in_dim(
        hidden_states.reshape(rows, model_width), vp_index * part, part, 0
    )
    size = part * groups
    total_rows = rows * groups
    blocks, full = call(
        first_kernel,
        "first",
        0,
        [
            jax.ShapeDtypeStruct((size, block), bf16),
            jax.ShapeDtypeStruct((total_rows, block), bf16),
        ],
        [pltpu.VMEM((part, model_width), bf16)] + sems(groups) + sems(groups) + spread_sems,
        mine,
        jnp.where(pipe_index == 0, layer_gain, gain_other),
    )
    for s in range(2):
        gain, up, down = section_of(s)
        hidden = jnp.dot(full, up, preferred_element_type=jnp.float32)
        piece = hidden.shape[0] // (2 * PIECES)
        active = call(
            chain_kernel,
            "chain",
            1,
            jax.ShapeDtypeStruct(hidden.shape, bf16),
            [pltpu.VMEM((2, PIECES, piece, half), jnp.float32)] * 2 + sems(2, PIECES) + sems(2, PIECES),
            hidden,
        )
        out = jnp.dot(active, down, preferred_element_type=jnp.float32)
        if s == 0:
            gain = section_of(1)[0]
            blocks, full = call(
                functools.partial(middle_kernel, model_width),
                "middle",
                2,
                [
                    jax.ShapeDtypeStruct((size, block), bf16),
                    jax.ShapeDtypeStruct((total_rows, block), bf16),
                ],
                buffers
                + [pltpu.VMEM((groups, 8, size), jnp.float32)]
                + reach_sems
                + sems(groups)
                + spread_sems,
                out,
                blocks,
                gain[None],
            )
        else:
            normed_final = call(
                last_kernel,
                "last",
                3,
                jax.ShapeDtypeStruct((rows, model_width), bf16),
                buffers
                + [pltpu.VMEM((size, block), bf16), pltpu.VMEM((groups, part, block), bf16)]
                + reach_sems
                + sems(groups)
                + spread_sems,
                out,
                blocks,
                final_gain[None],
            )
    logits = lax.dot_general(
        normed_final, unembedding, (((1,), (1,)), ((), ())), preferred_element_type=jnp.float32
    )
    vocab_start = vp_index * unembedding.shape[0]
    local_ids = target_ids.reshape(-1) - vocab_start
    columns = lax.broadcasted_iota(jnp.int32, logits.shape, 1)
    picked = jnp.sum(jnp.where(columns == local_ids[:, None], logits, 0.0), axis=1)
    local_top = jnp.max(logits, axis=1)
    local_sum = jnp.sum(jnp.exp(logits - local_top[:, None]), axis=1)
    stats = jnp.pad(jnp.stack([local_top, local_sum, picked]), ((0, 5), (0, 0)))
    padded = jnp.pad(local_counts[None], ((0, 7), (0, -seq_count % 128)))
    stats, counts = call(
        stats_kernel,
        "stats",
        4,
        [
            jax.ShapeDtypeStruct((vp_size * 8, rows), jnp.float32),
            jax.ShapeDtypeStruct(padded.shape, jnp.float32),
        ],
        [pltpu.VMEM((groups,) + padded.shape, jnp.float32)] + sems(groups) + spread_sems,
        stats,
        padded,
    )
    stats = stats.reshape(vp_size, 8, rows)
    counts = counts[0, :seq_count]
    top_value = jnp.max(stats[:, 0], axis=0)
    exp_total = jnp.sum(stats[:, 1] * jnp.exp(stats[:, 0] - top_value), axis=0)
    picked_all = jnp.sum(stats[:, 2], axis=0)
    token_logps = (picked_all - top_value - jnp.log(exp_total)).reshape(seq_count, length)

    divisor = jnp.repeat(counts / (groups * SEQ_MB), SEQ_MB)
    policy = jnp.sum(mask_values * token_logps, axis=1) / divisor
    anchor = jnp.sum(mask_values * anchor_logps, axis=1) / divisor
    log_gaps = policy - anchor
    positions = jnp.arange(seq_count, dtype=jnp.int32)
    chosen = jnp.sum(
        jnp.where(pairing[0, 0::2][:, None] == positions[None, :], log_gaps[None, :], 0.0), axis=1
    )
    rejected = jnp.sum(
        jnp.where(pairing[0, 1::2][:, None] == positions[None, :], log_gaps[None, :], 0.0), axis=1
    )
    losses = (chosen - rejected - 0.5 / ipo_tau) ** 2
    return (token_logps, policy, losses)


def solution(mesh):
    return jax.shard_map(
        shards,
        mesh=mesh,
        in_specs=(
            P("dp", None, None),
            P("pipe", "dp", "mp"),
            P("pipe", "mp", "dp"),
            P("pipe", None),
            P(),
            P(("pipe", "mp"), None),
            P("dp", None),
            P("dp", None),
            P("dp", None),
            P("dp", None),
        ),
        out_specs=(P("dp", None), P("dp"), P("dp")),
        check_vma=False,
    )
```
